256 devices in a mesh: grp: 2 (over z), kv: 128 (over y, x, core).
Axes of the slice: x: 8, y: 8, z: 2, core: 2. Of those that a mesh axis runs over, the one named last changes fastest.
The devices are a block of a 8x8x16 slice.
Arguments:
- queries: bfloat16 [1024, 40, 128], P(('grp', 'kv')), parts along dimension 0, may hold values from -250 to 250
- cache_keys: bfloat16 [65536, 40, 128], P(('grp', 'kv')), parts along dimension 0, may hold values from -8 to 8
- cache_values: bfloat16 [65536, 40, 128], P(('grp', 'kv')), parts along dimension 0, may hold values from -18 to 18
- new_keys: bfloat16 [1024, 40, 128], P(('grp', 'kv')), parts along dimension 0, may hold values from -4 to 4
- new_values: bfloat16 [1024, 40, 128], P(('grp', 'kv')), parts along dimension 0, may hold values from -4 to 4
- valid_frames: int32 [2], P('grp'), parts along dimension 0, may hold values from 64 to 128
Outputs:
- attended: bfloat16 [1024, 40, 128], P(('grp', 'kv')), parts along dimension 0
The draws below stay inside these ranges and needn't reach their ends.
There are 2 independent parts, one for each index of `grp`. The reference program is written for one: setup_inputs(seed, part) draws one part's arguments, and reference() takes and returns one part's arrays. A program takes and returns all parts, laid end to end along the dimension named above; each array names one. Nothing has to cross between parts.
All inputs are finite; a program needn't handle non-finite values.
Results may differ from the reference program's by a relative error of at most 0.0027.
Values may be sent and summed in bfloat16 or wider, within the bound.
A program may use at most 128 MiB of HBM per device.

```python
import math
import jax
import jax.numpy as jnp
from jax import lax

HEADS = 40
HEAD_DIM = 128
FRAME = 256
NEW = 512
CACHE = 32768
FRAMES = 128


def drawn_pair(key):
    base = jax.random.fold_in(key, 11)
    keys_all = jax.random.truncated_normal(jax.random.fold_in(base, 1), -4.0, 4.0, (CACHE, HEADS, HEAD_DIM), jnp.float32)
    query_all = 4.0 * jax.random.truncated_normal(jax.random.fold_in(base, 2), -4.0, 4.0, (NEW, HEADS, HEAD_DIM), jnp.float32)
    return (query_all, keys_all)


def draw_queries(key, part):
    return drawn_pair(key)[0].astype(jnp.bfloat16)


def draw_cache_keys(key, part):
    return drawn_pair(key)[1].astype(jnp.bfloat16)


def draw_cache_values(key, part):
    base = jax.random.fold_in(key, 23)
    values_all = jax.random.truncated_normal(jax.random.fold_in(base, 1), -4.0, 4.0, (CACHE, HEADS, HEAD_DIM), jnp.float32)
    return values_all.astype(jnp.bfloat16)


def shard_levels(own_key, dims, pieces, smallest, largest):
    def one(axis_at, blocks):
        draws = jax.random.uniform(jax.random.fold_in(jax.random.fold_in(own_key, 6), axis_at), (blocks,), jnp.float32, smallest / len(pieces), largest / len(pieces))
        return jnp.repeat(jnp.exp(draws), dims[axis_at] // blocks).reshape((-1,) + (1,) * (len(dims) - axis_at - 1))

    factor_of = one(*pieces[0])
    for cut in pieces[1:]:
        factor_of = factor_of * one(*cut)
    return factor_of


def noise(key, dims, deviation, reach, shards=(), kind=jnp.bfloat16):
    level = shard_levels(key, dims, shards, -0.22, 0.18) if shards else 1.0
    array = jax.random.normal(key, dims, jnp.float32) * deviation * level
    return jnp.minimum(jnp.maximum(array, -reach), reach).astype(kind)


def setup_inputs(seed: int = 0, part: int = 0) -> dict:
    arg_keys = jax.random.split(jax.random.key(seed), 7)
    part_keys = jax.random.split(jax.random.fold_in(arg_keys[6], part), 7)
    return {
        "queries": draw_queries(jax.random.fold_in(jax.random.fold_in(arg_keys[6], part), 71), part),
        "cache_keys": draw_cache_keys(jax.random.fold_in(jax.random.fold_in(arg_keys[6], part), 71), part),
        "cache_values": draw_cache_values(jax.random.fold_in(jax.random.fold_in(arg_keys[6], part), 71), part),
        "new_keys": noise(part_keys[3], (NEW, HEADS, HEAD_DIM), 1.0, 4.0, ((0, 128),)),
        "new_values": noise(part_keys[4], (NEW, HEADS, HEAD_DIM), 1.0, 4.0, ((0, 128),)),
        "valid_frames": jax.random.randint(part_keys[5], (1,), FRAMES // 2, FRAMES + 1).astype(jnp.int32),
    }


def reference(queries, cache_keys, cache_values, new_keys, new_values, valid_frames):
    limit = valid_frames[0] * FRAME
    positions = jnp.arange(CACHE, dtype=jnp.int32)
    live = positions < limit
    factor = 1.0 / math.sqrt(HEAD_DIM)

    def one_head(head):
        query_h = lax.dynamic_index_in_dim(queries, head, 1, keepdims=False)
        ckey_h = lax.dynamic_index_in_dim(cache_keys, head, 1, keepdims=False)
        cval_h = lax.dynamic_index_in_dim(cache_values, head, 1, keepdims=False)
        nkey_h = lax.dynamic_index_in_dim(new_keys, head, 1, keepdims=False)
        nval_h = lax.dynamic_index_in_dim(new_values, head, 1, keepdims=False)
        cache_score = jnp.dot(query_h, ckey_h.T, preferred_element_type=jnp.float32) * factor
        cache_score = jnp.where(live[None, :], cache_score, jnp.float32(-1e+30))
        new_score = jnp.dot(query_h, nkey_h.T, preferred_element_type=jnp.float32) * factor
        top = jnp.maximum(lax.optimization_barrier(jnp.max(cache_score, axis=1)), lax.optimization_barrier(jnp.max(new_score, axis=1)))
        cache_weight = jnp.exp(cache_score - top[:, None])
        new_weight = jnp.exp(new_score - top[:, None])
        total = lax.optimization_barrier(jnp.sum(cache_weight, axis=1)) + lax.optimization_barrier(jnp.sum(new_weight, axis=1))
        numerator = jnp.dot(cache_weight.astype(jnp.bfloat16), cval_h, preferred_element_type=jnp.float32)
        numerator = numerator + jnp.dot(new_weight.astype(jnp.bfloat16), nval_h, preferred_element_type=jnp.float32)
        return (numerator / total[:, None]).astype(jnp.bfloat16)
    result = lax.map(one_head, jnp.arange(HEADS, dtype=jnp.int32))
    return jnp.transpose(result, (1, 0, 2))
```

```python
import functools
import math

import jax
import jax.numpy as jnp
from jax import lax
from jax.experimental import pallas as pl
from jax.experimental.pallas import tpu as pltpu
from jax.sharding import Mesh
from jax.sharding import PartitionSpec as P

FRAME = 256
RING = (8, 8, 2)
GRP_KV = ("grp", "kv_0", "kv_1", "kv_2")
GROUPS = 5
RC = 32
PC = 512
NEG = -1e30
ROUTES = ((4, 2), (3, 1), (1, 1), (-3, -1), (-1, -1), (2, 2), (-2, -2))
BATCHES = ((0, 2), (2, 4), (4, 5))
LOG2E = math.log2(math.e)
TOP = 32767.0
MESH = pl.DeviceIdType.MESH
NT = (((1,), (1,)), ((), ()))


def steps_of(n, way):
    return n // 2 if way == 0 else n - 1 - n // 2


def plan():
    ny, nx, _ = RING
    ids, outs = {}, {}
    for name in ("q", "n", "k", "v", "fin"):
        ids[name] = len(ids)
        outs[name] = len(outs)
    for s in range(2):
        for m in range(nx):
            ids["p1", s, m] = len(ids)
        for e in range(nx // 2):
            for way in range(2):
                for k in range(steps_of(ny, way)):
                    ids["p2", s, e, way, k] = len(ids)
        for g in range(GROUPS):
            for t in range(len(ROUTES)):
                ids["p3", g, s, t] = len(ids)
            outs["p3", g, s] = len(outs)
        for b in range(len(BATCHES)):
            ids["p4", b, s] = len(ids)
            outs["p4", b, s] = len(outs)
        outs["ag", s] = len(outs)
    return ids, outs


def kernel(
    vf, q_hbm, k_hbm, v_hbm, nk_hbm, nv_hbm, out_ref,
    qraw, nraw, kraw, vraw, krel, vrel, kpart, vpart, nrel, qtmp, qbuf,
    score, weight, obuf, raw_stat, stat, rbuf, red, got,
    fin, finrecv, send_sem, recv_sem, local_sem,
):
    ny, nx, _ = RING
    ids, outs = plan()
    y, x, c = lax.axis_index("kv_0"), lax.axis_index("kv_1"), lax.axis_index("kv_2")
    pc = 1 - c
    tok, heads, dim = q_hbm.shape
    cached = k_hbm.shape[0]
    half = heads // 2
    per = half // (2 * GROUPS)
    chip_tok = 2 * tok
    coord = ((y, x), (x, y))
    n = ny
    rows = n * chip_tok
    queries = ny * nx * chip_tok
    c1 = LOG2E / math.sqrt(dim)
    partner = {"kv_2": pc}

    def device(s, major, minor):
        return {"kv_0": major if s == 0 else minor, "kv_1": minor if s == 0 else major}

    def remote(name, src, dst, dev, out=None, at=0):
        return pltpu.make_async_remote_copy(
            src_ref=src, dst_ref=dst,
            send_sem=send_sem.at[outs[name if out is None else out]],
            recv_sem=recv_sem.at[ids[name] + at], device_id=dev, device_id_type=MESH,
        )

    loads = [
        pltpu.make_async_copy(src, dst, local_sem.at[i])
        for i, (src, dst) in enumerate((
            (q_hbm, qraw.at[c]), (nk_hbm, nraw.at[c, 0]), (nv_hbm, nraw.at[c, 1]),
            (k_hbm, kraw), (v_hbm, vraw),
        ))
    ]
    for copy in loads:
        copy.start()
    barrier = pltpu.get_barrier_semaphore()
    peers = [partner]
    peers += [{"kv_0": lax.rem(y + d, ny)} for d in range(1, ny)]
    peers += [{"kv_1": lax.rem(x + d, nx)} for d in range(1, nx)]
    for dev in peers:
        pl.semaphore_signal(barrier, inc=1, device_id=dev, device_id_type=MESH)
    raw_stat[...] = jnp.zeros_like(raw_stat)
    nrel[...] = jnp.zeros_like(nrel)
    for i in range(3):
        loads[i].wait()
    pl.semaphore_wait(barrier, len(peers))

    qswap = remote("q", qraw.at[c], qraw.at[c], partner)
    qswap.start()
    nswap = remote("n", nraw.at[c], nraw.at[c], partner)
    nswap.start()

    def to_heads(value):
        wide = value.astype(jnp.float32)
        return [
            jnp.swapaxes(wide[:, h : h + 8], 0, 1).astype(jnp.bfloat16)
            for h in range(0, heads, 8)
        ]

    qswap.wait_recv()
    for i, part in enumerate(to_heads(qraw[...].reshape(chip_tok, heads, dim))):
        qtmp[8 * i : 8 * i + 8] = part

    for s in range(2):
        major, minor = coord[s]
        qbuf[s, major * n + minor] = qtmp[pl.ds(c * half + s * half // 2, half // 2)]

    def p1_copy(s, to, source):
        major, minor = coord[s]
        ref = qbuf.at[s, major * n + source]
        return remote(("p1", s, 0), ref, ref, device(s, major, to), ("ag", s), source)

    near = sorted(range(n), key=lambda d: min(d, n - d))
    for d in near[1:]:
        for s in range(2):
            minor = coord[s][1]
            p1_copy(s, lax.rem(minor + d, n), minor).start()

    def sign_of(i, way):
        return (1 if way == 0 else -1) * (1 if i % 2 == 0 else -1)

    def pair_at(s, e):
        return 2 * lax.rem(lax.div(coord[s][1], 2) + e, n // 2)

    def p2_copy(s, e, way, k):
        major, minor = coord[s]
        sign = sign_of(e, way)
        ref = qbuf.at[s, pl.ds(lax.rem(major - sign * k + n, n) * n + pair_at(s, e), 2)]
        dev = device(s, lax.rem(major + sign + n, n), minor)
        return remote(("p2", s, e, way, k), ref, ref, dev, ("ag", s))

    def p2_step(k, e):
        for s in range(2):
            minor = coord[s][1]
            if k == 0:
                if e == 0:
                    sibling = minor + 1 - 2 * lax.rem(minor, 2)
                    p1_copy(s, minor, sibling).wait_recv()
                else:
                    for one in range(2):
                        p1_copy(s, minor, pair_at(s, e) + one).wait_recv()
            for way in range(2):
                if 1 <= k <= steps_of(n, way):
                    p2_copy(s, e, way, k - 1).wait_recv()
                if k < steps_of(n, way):
                    p2_copy(s, e, way, k).start()

    gather = [
        functools.partial(p2_step, k, e) for k in range(steps_of(n, 0) + 1)
        for e in (0, 1, n // 2 - 1, 2)
    ]

    CH = 32

    def relayout(raw, rel, i):
        at = i * CH
        for j, piece in enumerate(to_heads(raw[at : at + CH])):
            rel[8 * j : 8 * j + 8, at : at + CH, :] = piece

    kswap = remote("k", krel.at[pl.ds(pc * half, half)], kpart, partner)
    vswap = remote("v", vrel.at[pl.ds(pc * half, half)], vpart, partner)

    def cache_part(raw, rel, load, swap, i):
        if i == 0:
            load.wait()
        relayout(raw, rel, i)
        if i == cached // CH - 1:
            swap.start()

    def news():
        nswap.wait_recv()
        for which in range(2):
            value = jnp.concatenate([nraw[0, which], nraw[1, which]], axis=0)
            for i, part in enumerate(to_heads(value)):
                nrel[which, 8 * i : 8 * i + 8, 0:chip_tok, :] = part

    prepare = [
        functools.partial(cache_part, kraw, krel, loads[3], kswap, i) for i in range(cached // CH)
    ]
    prepare += [
        functools.partial(cache_part, vraw, vrel, loads[4], vswap, i) for i in range(cached // CH)
    ]
    prepare += [news]

    def interleave(first, second, span):
        merged = sorted(
            [((i + 0.5) / len(first) * span, 0, i, f) for i, f in enumerate(first)]
            + [((i + 1.0) / len(second), 1, i, f) for i, f in enumerate(second)],
            key=lambda entry: entry[:3],
        )
        for entry in merged:
            entry[3]()

    interleave(prepare, gather, 0.8)
    kswap.wait_recv()
    vswap.wait_recv()

    index = (y * nx + x) * 2 + c
    live_own = index < vf[0]
    live_par = index + pc - c < vf[0]
    n_heads = half

    def split(i):
        g, r = lax.div(i, 2 * per), lax.rem(i, 2 * per)
        s, j = lax.div(r, per), lax.rem(r, per)
        return g, s, j, (s * GROUPS + g) * per + j

    def scores(i, slot):
        g, s, j, hh = split(i)
        q = qbuf[s, :, g * per + j].reshape(queries, dim)
        for key, lo in ((krel[c * half + hh], 0), (kpart[hh], cached), (nrel[0, c * half + hh], 2 * cached)):
            score[slot, :, lo : lo + key.shape[0]] = lax.dot_general(
                q, key, NT, preferred_element_type=jnp.float32
            )

    lane = lax.broadcasted_iota(jnp.int32, (8, 128), 1)

    def keep(which, i, r0, value):
        g, s, j, _ = split(i)
        for at in range(0, value.shape[0], rows):
            place, first = divmod(r0 + at, rows)
            acc = raw_stat[which, s * GROUPS + g, place]
            for r in range(0, min(rows, value.shape[0]), 8):
                mask = lane == 16 * ((first + r) // 8) + j
                acc = jnp.where(mask, jnp.broadcast_to(value[at + r : at + r + 8], (8, 128)), acc)
            raw_stat[which, s * GROUPS + g, place] = acc

    def softmax(i, slot):
        for r0 in range(0, queries, RC):
            so = score[slot, r0 : r0 + RC, 0:cached]
            sp = score[slot, r0 : r0 + RC, cached : 2 * cached]
            sn = score[slot, r0 : r0 + RC, 2 * cached : 2 * cached + 128]
            lanes = lax.broadcasted_iota(jnp.int32, sn.shape, 1)
            sn = jnp.where(lanes < chip_tok, sn, NEG)

            def fold(op, value):
                return op(value[:, :128], value[:, 128:])

            both = jnp.maximum(
                jnp.where(live_own, fold(jnp.maximum, so), NEG),
                jnp.where(live_par, fold(jnp.maximum, sp), NEG),
            )
            top = jnp.max(jnp.maximum(both, sn), axis=1, keepdims=True)
            po = jnp.exp2((so - jnp.where(live_own, top, -NEG)) * c1)
            pp = jnp.exp2((sp - jnp.where(live_par, top, -NEG)) * c1)
            pn = jnp.exp2((sn - top) * c1)
            total = jnp.sum(
                fold(jnp.add, po) + fold(jnp.add, pp) + pn, axis=1, keepdims=True
            )
            weight[slot, r0 : r0 + RC, 0:cached] = po.astype(jnp.bfloat16)
            weight[slot, r0 : r0 + RC, cached : 2 * cached] = pp.astype(jnp.bfloat16)
            weight[slot, r0 : r0 + RC, 2 * cached :] = pn.astype(jnp.bfloat16)
            keep(0, i, r0, top)
            keep(1, i, r0, total)

    def values(i, slot):
        hh = split(i)[3]
        for r0 in range(0, queries, PC):
            o = None
            for value, lo in ((vrel[c * half + hh], 0), (vpart[hh], cached), (nrel[1, c * half + hh], 2 * cached)):
                term = jnp.dot(
                    weight[slot, r0 : r0 + PC, lo : lo + value.shape[0]], value,
                    preferred_element_type=jnp.float32,
                )
                o = term if o is None else o + term
            big = jnp.maximum(jnp.max(jnp.abs(o), axis=1, keepdims=True), 1e-30)
            o = pack(o * (TOP / big))
            g, s, j, _ = split(i)
            for r in range(0, PC, rows):
                to = pl.ds(pl.multiple_of(j * rows, rows), rows)
                obuf[s * GROUPS + g, (r0 + r) // rows, to, :] = o[r : r + rows]
            keep(2, i, r0, big)

    def pack(value):
        return jnp.round(value).astype(jnp.int32).astype(jnp.int16)

    def unpack(value):
        return value.astype(jnp.int32).astype(jnp.float32)

    place16 = lane % 16
    FINE = 32768.0

    def encode(level, size):
        level_whole, size_whole = jnp.floor(level), jnp.floor(size)
        level_rest = jnp.floor((level - level_whole) * FINE)
        size_rest = jnp.floor((size - size_whole) * FINE)
        low = jnp.where(place16 < 4, level_whole, pltpu.roll(level_rest, 4, 1))
        high = jnp.where(place16 < 12, pltpu.roll(size_whole, 8, 1), pltpu.roll(size_rest, 12, 1))
        return jnp.where(place16 < 8, low, high).astype(jnp.int32).astype(jnp.int16)

    def decode(value):
        level = value + pltpu.roll(value, 124, 1) * (1 / FINE)
        return level, pltpu.roll(level, 120, 1)

    def settle(g):
        for s in range(2):
            gs = s * GROUPS + g
            for place in range(n):
                total = jnp.log(jnp.maximum(raw_stat[1, gs, place], 1e-37)) * LOG2E
                big = jnp.log(jnp.maximum(raw_stat[2, gs, place], 1e-37)) * LOG2E
                level, size = raw_stat[0, gs, place] * c1 + total, big - total
                stat[gs, place, 0] = level
                stat[gs, place, 1] = size
                obuf[gs, place, per * rows :, :] = encode(level, size)

    def combine(pairs):
        top = functools.reduce(jnp.maximum, [level for level, _ in pairs])
        total = functools.reduce(jnp.add, [jnp.exp2(level - top) for level, _ in pairs])
        level = top + jnp.log(total) * LOG2E
        both = [one + size for one, size in pairs]
        most = functools.reduce(jnp.maximum, both)
        parts = [jnp.exp2(one - most) for one in both]
        whole = functools.reduce(jnp.add, parts)
        size = most + jnp.log(whole) * LOG2E - level
        inverse = 1.0 / whole
        return level, size, [part * inverse for part in parts]

    def spread(packed, j, groups):
        one = [
            jnp.broadcast_to(packed[:, 16 * i + j : 16 * i + j + 1], (8, 128)) for i in range(groups)
        ]
        return one[0] if groups == 1 else jnp.concatenate(one, axis=0)

    def slot_of(g, s, t):
        return (2 * g + s) * len(ROUTES) + t

    def along(g, s, steps):
        return lax.rem(coord[s][0] + (steps if g % 2 == 0 else -steps) + n, n)

    def p3_copy(g, s, t, src):
        dev = device(s, along(g, s, ROUTES[t][1]), coord[s][1])
        return remote(("p3", g, s, t), src, rbuf.at[slot_of(g, s, t)], dev, ("p3", g, s))

    per4 = per * chip_tok + 8

    def part_of(g, s, dest):
        gs = s * GROUPS + g
        return obuf.at[gs, dest], (stat[gs, dest, 0], stat[gs, dest, 1])

    def merged(g, s, dest, slots):
        own, own_stat = part_of(g, s, dest)
        pairs = [own_stat] + [decode(unpack(rbuf[at, per * rows :, :])) for at in slots]
        level, size, shares = combine(pairs)
        data = []
        for j in range(per):
            at = pl.ds(j * rows, rows)
            mine = unpack(own[at, :])
            value = mine
            for slot, share in zip(slots, shares[1:]):
                value = value + spread(share, j, n) * (unpack(rbuf[slot, at, :]) - mine)
            data.append(pack(value))
        return data, encode(level, size)

    def p3_step(g, k):
        if k == 0:
            for t in (0, 3, 1, 2, 4):
                for s in range(2):
                    p3_copy(g, s, t, part_of(g, s, along(g, s, ROUTES[t][0]))[0]).start()
            return
        if k == 1:
            for t in (0, 3, 1):
                for s in range(2):
                    p3_copy(g, s, t, rbuf.at[slot_of(g, s, t)]).wait_recv()
            for s in range(2):
                for t, into, sources in ((5, 0, (0, 1)), (6, 3, (3,))):
                    slots = [slot_of(g, s, source) for source in sources]
                    data, code = merged(g, s, along(g, s, ROUTES[t][0]), slots)
                    at = slot_of(g, s, into)
                    for j in range(per):
                        rbuf[at, j * rows : (j + 1) * rows, :] = data[j]
                    rbuf[at, per * rows :, :] = code
            for t, into in ((5, 0), (6, 3)):
                for s in range(2):
                    p3_copy(g, s, t, rbuf.at[slot_of(g, s, into)]).start()
            return
        for t in (2, 4, 5, 6):
            for s in range(2):
                p3_copy(g, s, t, rbuf.at[slot_of(g, s, t)]).wait_recv()
        for s in range(2):
            data, code = merged(g, s, coord[s][0], [slot_of(g, s, t) for t in (2, 4, 5, 6)])
            for m in range(n):
                for j in range(per):
                    at = g * per4 + j * chip_tok
                    red[s, m, at : at + chip_tok, :] = data[j][m * chip_tok : (m + 1) * chip_tok]
                at = g * per4 + per * chip_tok
                red[s, m, at : at + 8, :] = code
        for b, (g0, g1) in enumerate(BATCHES):
            if g == g1 - 1:
                for d in near[:0:-1]:
                    for s in range(2):
                        p4_copy(b, s, d).start()

    def p4_copy(b, s, d):
        major, minor = coord[s]
        to = lax.rem(minor + d, n)
        part = pl.ds(BATCHES[b][0] * per4, (BATCHES[b][1] - BATCHES[b][0]) * per4)
        return remote(
            ("p4", b, s), red.at[s, to, part, :], got.at[s, d - 1, part, :], device(s, major, to)
        )

    def all_of(ref, sem):
        pltpu.make_async_copy(ref, ref, sem).wait()

    def p4_finish(b):
        g0, g1 = BATCHES[b]
        part = pl.ds(g0 * per4, (g1 - g0) * per4)
        for s in range(2):
            all_of(got.at[s, 0 : n - 1, part, :], recv_sem.at[ids["p4", b, s]])
        for s in range(2):
            major, minor = coord[s]
            shift = lax.rem(128 - 16 * minor, 128)
            for g in range(g0, g1):
                first = g * per4
                sources = [red.at[s, minor]] + [got.at[s, d] for d in range(n - 1)]
                pairs = []
                for source in sources:
                    code = unpack(source[first + per * chip_tok : first + per4, :])
                    pairs.append(decode(pltpu.roll(code, shift, 1)))
                top = functools.reduce(jnp.maximum, [level for level, _ in pairs])
                total = functools.reduce(jnp.add, [jnp.exp2(level - top) for level, _ in pairs])
                inverse = 1.0 / (total * TOP)
                parts = [jnp.exp2((level - top) + size) * inverse for level, size in pairs]
                for j in range(per):
                    at = first + j * chip_tok
                    terms = [
                        unpack(source[at : at + chip_tok, :]) * spread(p, j, 1)
                        for source, p in zip(sources, parts)
                    ]
                    fin[(s * GROUPS + g) * per + j] = functools.reduce(jnp.add, terms)

    last = n_heads - 1
    ahead = lambda i: jnp.minimum(i, last)
    scores(0, 0)
    scores(1, 1)
    softmax(0, 0)
    for g in range(GROUPS):
        first = g * 2 * per + 1

        def pair(t, carry):
            i = first + 2 * t
            scores(ahead(i + 1), 0)
            softmax(i, 1)
            values(i - 1, 0)
            scores(ahead(i + 2), 1)
            softmax(ahead(i + 1), 0)
            values(i, 1)
            return carry

        lax.fori_loop(0, per, pair, 0)
        settle(g)
        for gg in range(g, max(g - 3, -1), -1):
            p3_step(gg, g - gg)
    p3_step(GROUPS - 1, 1)
    p3_step(GROUPS - 2, 2)
    p4_finish(0)
    p3_step(GROUPS - 1, 2)
    for b in range(1, len(BATCHES)):
        p4_finish(b)

    tokens = jnp.swapaxes(fin[...], 0, 1)
    qt = jnp.where(c == 0, tokens[:tok], tokens[tok:])
    ot = jnp.where(c == 0, tokens[tok:], tokens[:tok])
    finrecv[0] = ot
    fswap = remote("fin", finrecv.at[0], finrecv.at[1], partner)
    fswap.start()
    fswap.wait_recv()
    theirs = finrecv[1]
    low = jnp.where(c == 0, qt, theirs)
    high = jnp.where(c == 0, theirs, qt)
    out_ref[...] = jnp.concatenate([low, high], axis=1).astype(out_ref.dtype)
    for swap in (qswap, nswap, kswap, vswap, fswap):
        swap.wait_send()
    for s in range(2):
        all_of(qbuf.at[s, 0 : n * n - 1], send_sem.at[outs["ag", s]])
        for g in range(GROUPS):
            all_of(obuf.at[s * GROUPS + g, 0 : n - 1], send_sem.at[outs["p3", g, s]])
        for b, (g0, g1) in enumerate(BATCHES):
            part = pl.ds(g0 * per4, (g1 - g0) * per4)
            all_of(got.at[s, 0 : n - 1, part, :], send_sem.at[outs["p4", b, s]])


def per_device(queries, cache_keys, cache_values, new_keys, new_values, valid_frames):
    ny, nx, _ = RING
    tok, heads, dim = queries.shape
    cached = cache_keys.shape[0]
    assert cached == FRAME and ny == nx == 8
    half = heads // 2
    per = half // (2 * GROUPS)
    chip_tok = 2 * tok
    total = ny * nx * chip_tok
    rows = nx * chip_tok
    ids, outs = plan()
    bf16, i16, f32 = jnp.bfloat16, jnp.int16, jnp.float32
    vmem = pltpu.VMEM
    return pl.pallas_call(
        kernel,
        name="stream_attention",
        out_shape=jax.ShapeDtypeStruct((tok, heads, dim), jnp.bfloat16),
        in_specs=[pl.BlockSpec(memory_space=pltpu.SMEM)]
        + [pl.BlockSpec(memory_space=pl.ANY)] * 5,
        out_specs=pl.BlockSpec(memory_space=pltpu.VMEM),
        scratch_shapes=[
            vmem((2, tok, heads, dim), bf16),
            vmem((2, 2, tok, heads, dim), bf16),
            vmem((cached, heads, dim), bf16),
            vmem((cached, heads, dim), bf16),
            vmem((heads, cached, dim), bf16),
            vmem((heads, cached, dim), bf16),
            vmem((half, cached, dim), bf16),
            vmem((half, cached, dim), bf16),
            vmem((2, heads, 128, dim), bf16),
            vmem((heads, chip_tok, dim), bf16),
            vmem((2, ny * nx, half // 2, chip_tok, dim), bf16),
            vmem((2, total, 2 * cached + 128), f32),
            vmem((2, total, 2 * cached + 128), bf16),
            vmem((2 * GROUPS, ny, per * rows + 8, dim), i16),
            vmem((3, 2 * GROUPS, ny, 8, 128), f32),
            vmem((2 * GROUPS, ny, 2, 8, 128), f32),
            vmem((2 * GROUPS * len(ROUTES), per * rows + 8, dim), i16),
            vmem((2, nx, GROUPS * (per * chip_tok + 8), dim), i16),
            vmem((2, nx - 1, GROUPS * (per * chip_tok + 8), dim), i16),
            vmem((half, chip_tok, dim), f32),
            vmem((2, tok, half, dim), f32),
            pltpu.SemaphoreType.DMA((len(outs),)),
            pltpu.SemaphoreType.DMA((len(ids),)),
            pltpu.SemaphoreType.DMA((5,)),
        ],
        compiler_params=pltpu.CompilerParams(
            collective_id=0, has_side_effects=True, vmem_limit_bytes=60 * 1024 * 1024
        ),
    )(valid_frames, queries, cache_keys, cache_values, new_keys, new_values)


def solution(mesh):
    torus = Mesh(mesh.devices.reshape(mesh.shape["grp"], *RING), GRP_KV)
    return jax.shard_map(
        per_device,
        mesh=torus,
        in_specs=(P(GRP_KV, None, None),) * 5 + (P("grp"),),
        out_specs=P(GRP_KV, None, None),
        check_vma=False,
    )
```

```python
import functools
import math

import jax
import jax.numpy as jnp
from jax import lax
from jax.experimental import pallas as pl
from jax.experimental.pallas import tpu as pltpu
from jax.sharding import Mesh
from jax.sharding import PartitionSpec as P

FRAME = 256
RING = (8, 8, 2)
GRP_KV = ("grp", "kv_0", "kv_1", "kv_2")
GROUPS = 5
RC = 32
PC = 512
NEG = -1e30
ROUTES = ((4, 2), (3, 1), (1, 1), (-3, -1), (-1, -1), (2, 2), (-2, -2))
BATCHES = ((0, 2), (2, 4), (4, 5))
LOG2E = math.log2(math.e)
TOP = 32767.0
MESH = pl.DeviceIdType.MESH
NT = (((1,), (1,)), ((), ()))


def steps_of(n, way):
    return n // 2 if way == 0 else n - 1 - n // 2


def plan():
    ny, nx, _ = RING
    ids, outs = {}, {}
    for name in ("q", "n", "k", "v", "fin"):
        ids[name] = len(ids)
        outs[name] = len(outs)
    for s in range(2):
        for m in range(nx):
            ids["p1", s, m] = len(ids)
        for e in range(nx // 2):
            for way in range(2):
                for k in range(steps_of(ny, way)):
                    ids["p2", s, e, way, k] = len(ids)
        for g in range(GROUPS):
            for t in range(len(ROUTES)):
                ids["p3", g, s, t] = len(ids)
            outs["p3", g, s] = len(outs)
        for b in range(len(BATCHES)):
            ids["p4", b, s] = len(ids)
            outs["p4", b, s] = len(outs)
        outs["ag", s] = len(outs)
    return ids, outs


def kernel(
    vf, q_hbm, k_hbm, v_hbm, nk_hbm, nv_hbm, out_ref,
    qraw, nraw, kraw, vraw, krel, vrel, kpart, vpart, nrel, qtmp, qbuf,
    score, weight, obuf, raw_stat, stat, rbuf, red, got,
    fin, finrecv, send_sem, recv_sem, local_sem,
):
    ny, nx, _ = RING
    ids, outs = plan()
    y, x, c = lax.axis_index("kv_0"), lax.axis_index("kv_1"), lax.axis_index("kv_2")
    pc = 1 - c
    tok, heads, dim = q_hbm.shape
    cached = k_hbm.shape[0]
    half = heads // 2
    per = half // (2 * GROUPS)
    chip_tok = 2 * tok
    coord = ((y, x), (x, y))
    n = ny
    rows = n * chip_tok
    queries = ny * nx * chip_tok
    c1 = LOG2E / math.sqrt(dim)
    partner = {"kv_2": pc}

    def device(s, major, minor):
        return {"kv_0": major if s == 0 else minor, "kv_1": minor if s == 0 else major}

    def remote(name, src, dst, dev, out=None, at=0):
        return pltpu.make_async_remote_copy(
            src_ref=src, dst_ref=dst,
            send_sem=send_sem.at[outs[name if out is None else out]],
            recv_sem=recv_sem.at[ids[name] + at], device_id=dev, device_id_type=MESH,
        )

    loads = [
        pltpu.make_async_copy(src, dst, local_sem.at[i])
        for i, (src, dst) in enumerate((
            (q_hbm, qraw.at[c]), (nk_hbm, nraw.at[c, 0]), (nv_hbm, nraw.at[c, 1]),
            (k_hbm, kraw), (v_hbm, vraw),
        ))
    ]
    for copy in loads:
        copy.start()
    barrier = pltpu.get_barrier_semaphore()
    peers = [partner]
    peers += [{"kv_0": lax.rem(y + d, ny)} for d in range(1, ny)]
    peers += [{"kv_1": lax.rem(x + d, nx)} for d in range(1, nx)]
    for dev in peers:
        pl.semaphore_signal(barrier, inc=1, device_id=dev, device_id_type=MESH)
    raw_stat[...] = jnp.zeros_like(raw_stat)
    nrel[...] = jnp.zeros_like(nrel)
    for i in range(3):
        loads[i].wait()
    pl.semaphore_wait(barrier, len(peers))

    qswap = remote("q", qraw.at[c], qraw.at[c], partner)
    qswap.start()
    nswap = remote("n", nraw.at[c], nraw.at[c], partner)
    nswap.start()

    def to_heads(value):
        wide = value.astype(jnp.float32)
        return [
            jnp.swapaxes(wide[:, h : h + 8], 0, 1).astype(jnp.bfloat16)
            for h in range(0, heads, 8)
        ]

    qswap.wait_recv()
    for i, part in enumerate(to_heads(qraw[...].reshape(chip_tok, heads, dim))):
        qtmp[8 * i : 8 * i + 8] = part

    for s in range(2):
        major, minor = coord[s]
        qbuf[s, major * n + minor] = qtmp[pl.ds(c * half + s * half // 2, half // 2)]

    def p1_copy(s, to, source):
        major, minor = coord[s]
        ref = qbuf.at[s, major * n + source]
        return remote(("p1", s, 0), ref, ref, device(s, major, to), ("ag", s), source)

    near = sorted(range(n), key=lambda d: min(d, n - d))
    for d in near[1:]:
        for s in range(2):
            minor = coord[s][1]
            p1_copy(s, lax.rem(minor + d, n), minor).start()

    def sign_of(i, way):
        return (1 if way == 0 else -1) * (1 if i % 2 == 0 else -1)

    def pair_at(s, e):
        return 2 * lax.rem(lax.div(coord[s][1], 2) + e, n // 2)

    def p2_copy(s, e, way, k):
        major, minor = coord[s]
        sign = sign_of(e, way)
        ref = qbuf.at[s, pl.ds(lax.rem(major - sign * k + n, n) * n + pair_at(s, e), 2)]
        dev = device(s, lax.rem(major + sign + n, n), minor)
        return remote(("p2", s, e, way, k), ref, ref, dev, ("ag", s))

    def p2_step(k, e):
        for s in range(2):
            minor = coord[s][1]
            if k == 0:
                if e == 0:
                    sibling = minor + 1 - 2 * lax.rem(minor, 2)
                    p1_copy(s, minor, sibling).wait_recv()
                else:
                    for one in range(2):
                        p1_copy(s, minor, pair_at(s, e) + one).wait_recv()
            for way in range(2):
                if 1 <= k <= steps_of(n, way):
                    p2_copy(s, e, way, k - 1).wait_recv()
                if k < steps_of(n, way):
                    p2_copy(s, e, way, k).start()

    gather = [
        functools.partial(p2_step, k, e) for k in range(steps_of(n, 0) + 1)
        for e in (0, 1, n // 2 - 1, 2)
    ]

    CH = 32

    def relayout(raw, rel, i):
        at = i * CH
        for j, piece in enumerate(to_heads(raw[at : at + CH])):
            rel[8 * j : 8 * j + 8, at : at + CH, :] = piece

    kswap = remote("k", krel.at[pl.ds(pc * half, half)], kpart, partner)
    vswap = remote("v", vrel.at[pl.ds(pc * half, half)], vpart, partner)

    def cache_part(raw, rel, load, swap, i):
        if i == 0:
            load.wait()
        relayout(raw, rel, i)
        if i == cached // CH - 1:
            swap.start()

    def news():
        nswap.wait_recv()
        for which in range(2):
            value = jnp.concatenate([nraw[0, which], nraw[1, which]], axis=0)
            for i, part in enumerate(to_heads(value)):
                nrel[which, 8 * i : 8 * i + 8, 0:chip_tok, :] = part

    prepare = [
        functools.partial(cache_part, kraw, krel, loads[3], kswap, i) for i in range(cached // CH)
    ]
    prepare += [
        functools.partial(cache_part, vraw, vrel, loads[4], vswap, i) for i in range(cached // CH)
    ]
    prepare += [news]

    def interleave(first, second, span):
        merged = sorted(
            [((i + 0.5) / len(first) * span, 0, i, f) for i, f in enumerate(first)]
            + [((i + 1.0) / len(second), 1, i, f) for i, f in enumerate(second)],
            key=lambda entry: entry[:3],
        )
        for entry in merged:
            entry[3]()

    interleave(prepare, gather, 0.8)
    kswap.wait_recv()
    vswap.wait_recv()

    index = (y * nx + x) * 2 + c
    live_own = index < vf[0]
    live_par = index + pc - c < vf[0]
    n_heads = half

    def split(i):
        g, r = lax.div(i, 2 * per), lax.rem(i, 2 * per)
        s, j = lax.div(r, per), lax.rem(r, per)
        return g, s, j, (s * GROUPS + g) * per + j

    def scores(i, slot):
        g, s, j, hh = split(i)
        q = qbuf[s, :, g * per + j].reshape(queries, dim)
        for key, lo in ((krel[c * half + hh], 0), (kpart[hh], cached), (nrel[0, c * half + hh], 2 * cached)):
            score[slot, :, lo : lo + key.shape[0]] = lax.dot_general(
                q, key, NT, preferred_element_type=jnp.float32
            )

    lane = lax.broadcasted_iota(jnp.int32, (8, 128), 1)

    def keep(which, i, r0, value):
        g, s, j, _ = split(i)
        for at in range(0, value.shape[0], rows):
            place, first = divmod(r0 + at, rows)
            acc = raw_stat[which, s * GROUPS + g, place]
            for r in range(0, min(rows, value.shape[0]), 8):
                mask = lane == 16 * ((first + r) // 8) + j
                acc = jnp.where(mask, jnp.broadcast_to(value[at + r : at + r + 8], (8, 128)), acc)
            raw_stat[which, s * GROUPS + g, place] = acc

    def softmax(i, slot):
        for r0 in range(0, queries, RC):
            so = score[slot, r0 : r0 + RC, 0:cached]
            sp = score[slot, r0 : r0 + RC, cached : 2 * cached]
            sn = score[slot, r0 : r0 + RC, 2 * cached : 2 * cached + 128]
            lanes = lax.broadcasted_iota(jnp.int32, sn.shape, 1)
            sn = jnp.where(lanes < chip_tok, sn, NEG)

            def fold(op, value):
                return op(value[:, :128], value[:, 128:])

            both = jnp.maximum(
                jnp.where(live_own, fold(jnp.maximum, so), NEG),
                jnp.where(live_par, fold(jnp.maximum, sp), NEG),
            )
            top = jnp.max(jnp.maximum(both, sn), axis=1, keepdims=True)
            po = jnp.exp2((so - jnp.where(live_own, top, -NEG)) * c1)
            pp = jnp.exp2((sp - jnp.where(live_par, top, -NEG)) * c1)
            pn = jnp.exp2((sn - top) * c1)
            total = jnp.sum(
                fold(jnp.add, po) + fold(jnp.add, pp) + pn, axis=1, keepdims=True
            )
            weight[slot, r0 : r0 + RC, 0:cached] = po.astype(jnp.bfloat16)
            weight[slot, r0 : r0 + RC, cached : 2 * cached] = pp.astype(jnp.bfloat16)
            weight[slot, r0 : r0 + RC, 2 * cached :] = pn.astype(jnp.bfloat16)
            keep(0, i, r0, top)
            keep(1, i, r0, total)

    def values(i, slot):
        hh = split(i)[3]
        for r0 in range(0, queries, PC):
            o = None
            for value, lo in ((vrel[c * half + hh], 0), (vpart[hh], cached), (nrel[1, c * half + hh], 2 * cached)):
                term = jnp.dot(
                    weight[slot, r0 : r0 + PC, lo : lo + value.shape[0]], value,
                    preferred_element_type=jnp.float32,
                )
                o = term if o is None else o + term
            big = jnp.maximum(jnp.max(jnp.abs(o), axis=1, keepdims=True), 1e-30)
            o = pack(o * (TOP / big))
            g, s, j, _ = split(i)
            for r in range(0, PC, rows):
                to = pl.ds(pl.multiple_of(j * rows, rows), rows)
                obuf[s * GROUPS + g, (r0 + r) // rows, to, :] = o[r : r + rows]
            keep(2, i, r0, big)

    def pack(value):
        return jnp.round(value).astype(jnp.int32).astype(jnp.int16)

    def unpack(value):
        return value.astype(jnp.int32).astype(jnp.float32)

    place16 = lane % 16
    FINE = 32768.0

    def encode(level, size):
        level_whole, size_whole = jnp.floor(level), jnp.floor(size)
        level_rest = jnp.floor((level - level_whole) * FINE)
        size_rest = jnp.floor((size - size_whole) * FINE)
        low = jnp.where(place16 < 4, level_whole, pltpu.roll(level_rest, 4, 1))
        high = jnp.where(place16 < 12, pltpu.roll(size_whole, 8, 1), pltpu.roll(size_rest, 12, 1))
        return jnp.where(place16 < 8, low, high).astype(jnp.int32).astype(jnp.int16)

    def decode(value):
        level = value + pltpu.roll(value, 124, 1) * (1 / FINE)
        return level, pltpu.roll(level, 120, 1)

    def settle(g):
        for s in range(2):
            gs = s * GROUPS + g
            for place in range(n):
                total = jnp.log(jnp.maximum(raw_stat[1, gs, place], 1e-37)) * LOG2E
                big = jnp.log(jnp.maximum(raw_stat[2, gs, place], 1e-37)) * LOG2E
                level, size = raw_stat[0, gs, place] * c1 + total, big - total
                stat[gs, place, 0] = level
                stat[gs, place, 1] = size
                obuf[gs, place, per * rows :, :] = encode(level, size)

    def combine(pairs):
        top = functools.reduce(jnp.maximum, [level for level, _ in pairs])
        total = functools.reduce(jnp.add, [jnp.exp2(level - top) for level, _ in pairs])
        level = top + jnp.log(total) * LOG2E
        both = [one + size for one, size in pairs]
        most = functools.reduce(jnp.maximum, both)
        parts = [jnp.exp2(one - most) for one in both]
        whole = functools.reduce(jnp.add, parts)
        size = most + jnp.log(whole) * LOG2E - level
        inverse = 1.0 / whole
        return level, size, [part * inverse for part in parts]

    def spread(packed, j, groups):
        one = [
            jnp.broadcast_to(packed[:, 16 * i + j : 16 * i + j + 1], (8, 128)) for i in range(groups)
        ]
        return one[0] if groups == 1 else jnp.concatenate(one, axis=0)

    def slot_of(g, s, t):
        return (2 * g + s) * len(ROUTES) + t

    def along(g, s, steps):
        return lax.rem(coord[s][0] + (steps if g % 2 == 0 else -steps) + n, n)

    def p3_copy(g, s, t, src):
        dev = device(s, along(g, s, ROUTES[t][1]), coord[s][1])
        return remote(("p3", g, s, t), src, rbuf.at[slot_of(g, s, t)], dev, ("p3", g, s))

    per4 = per * chip_tok + 8

    def part_of(g, s, dest):
        gs = s * GROUPS + g
        return obuf.at[gs, dest], (stat[gs, dest, 0], stat[gs, dest, 1])

    def merged(g, s, dest, slots):
        own, own_stat = part_of(g, s, dest)
        pairs = [own_stat] + [decode(unpack(rbuf[at, per * rows :, :])) for at in slots]
        level, size, shares = combine(pairs)
        data = []
        for j in range(per):
            at = pl.ds(j * rows, rows)
            mine = unpack(own[at, :])
            value = mine
            for slot, share in zip(slots, shares[1:]):
                value = value + spread(share, j, n) * (unpack(rbuf[slot, at, :]) - mine)
            data.append(pack(value))
        return data, encode(level, size)

    def p3_step(g, k):
        if k == 0:
            for t in (0, 3, 1, 2, 4):
                for s in range(2):
                    p3_copy(g, s, t, part_of(g, s, along(g, s, ROUTES[t][0]))[0]).start()
            return
        if k == 1:
            for t in (0, 3, 1):
                for s in range(2):
                    p3_copy(g, s, t, rbuf.at[slot_of(g, s, t)]).wait_recv()
            for s in range(2):
                for t, into, sources in ((5, 0, (0, 1)), (6, 3, (3,))):
                    slots = [slot_of(g, s, source) for source in sources]
                    data, code = merged(g, s, along(g, s, ROUTES[t][0]), slots)
                    at = slot_of(g, s, into)
                    for j in range(per):
                        rbuf[at, j * rows : (j + 1) * rows, :] = data[j]
                    rbuf[at, per * rows :, :] = code
            for t, into in ((5, 0), (6, 3)):
                for s in range(2):
                    p3_copy(g, s, t, rbuf.at[slot_of(g, s, into)]).start()
            return
        for t in (2, 4, 5, 6):
            for s in range(2):
                p3_copy(g, s, t, rbuf.at[slot_of(g, s, t)]).wait_recv()
        for s in range(2):
            data, code = merged(g, s, coord[s][0], [slot_of(g, s, t) for t in (2, 4, 5, 6)])
            for m in range(n):
                for j in range(per):
                    at = g * per4 + j * chip_tok
                    red[s, m, at : at + chip_tok, :] = data[j][m * chip_tok : (m + 1) * chip_tok]
                at = g * per4 + per * chip_tok
                red[s, m, at : at + 8, :] = code
        for b, (g0, g1) in enumerate(BATCHES):
            if g == g1 - 1:
                for d in near[:0:-1]:
                    for s in range(2):
                        p4_copy(b, s, d).start()

    def p4_copy(b, s, d):
        major, minor = coord[s]
        to = lax.rem(minor + d, n)
        part = pl.ds(BATCHES[b][0] * per4, (BATCHES[b][1] - BATCHES[b][0]) * per4)
        return remote(
            ("p4", b, s), red.at[s, to, part, :], got.at[s, d - 1, part, :], device(s, major, to)
        )

    def all_of(ref, sem):
        pltpu.make_async_copy(ref, ref, sem).wait()

    def p4_finish(b):
        g0, g1 = BATCHES[b]
        part = pl.ds(g0 * per4, (g1 - g0) * per4)
        for s in range(2):
            all_of(got.at[s, 0 : n - 1, part, :], recv_sem.at[ids["p4", b, s]])
        for s in range(2):
            major, minor = coord[s]
            shift = lax.rem(128 - 16 * minor, 128)
            for g in range(g0, g1):
                first = g * per4
                sources = [red.at[s, minor]] + [got.at[s, d] for d in range(n - 1)]
                pairs = []
                for source in sources:
                    code = unpack(source[first + per * chip_tok : first + per4, :])
                    pairs.append(decode(pltpu.roll(code, shift, 1)))
                top = functools.reduce(jnp.maximum, [level for level, _ in pairs])
                total = functools.reduce(jnp.add, [jnp.exp2(level - top) for level, _ in pairs])
                inverse = 1.0 / (total * TOP)
                parts = [jnp.exp2((level - top) + size) * inverse for level, size in pairs]
                for j in range(per):
                    at = first + j * chip_tok
                    terms = [
                        unpack(source[at : at + chip_tok, :]) * spread(p, j, 1)
                        for source, p in zip(sources, parts)
                    ]
                    fin[(s * GROUPS + g) * per + j] = functools.reduce(jnp.add, terms)

    last = n_heads - 1
    ahead = lambda i: jnp.minimum(i, last)
    scores(0, 0)
    scores(1, 1)
    softmax(0, 0)
    for g in range(GROUPS):
        first = g * 2 * per + 1

        def pair(t, carry):
            i = first + 2 * t
            scores(ahead(i + 1), 0)
            softmax(i, 1)
            values(i - 1, 0)
            scores(ahead(i + 2), 1)
            softmax(ahead(i + 1), 0)
            values(i, 1)
            return carry

        for t in range(per):
            pair(t, 0)
        settle(g)
        for gg in range(g, max(g - 3, -1), -1):
            p3_step(gg, g - gg)
    p3_step(GROUPS - 1, 1)
    p3_step(GROUPS - 2, 2)
    p4_finish(0)
    p3_step(GROUPS - 1, 2)
    for b in range(1, len(BATCHES)):
        p4_finish(b)

    tokens = jnp.swapaxes(fin[...], 0, 1)
    qt = jnp.where(c == 0, tokens[:tok], tokens[tok:])
    ot = jnp.where(c == 0, tokens[tok:], tokens[:tok])
    finrecv[0] = ot
    fswap = remote("fin", finrecv.at[0], finrecv.at[1], partner)
    fswap.start()
    fswap.wait_recv()
    theirs = finrecv[1]
    low = jnp.where(c == 0, qt, theirs)
    high = jnp.where(c == 0, theirs, qt)
    out_ref[...] = jnp.concatenate([low, high], axis=1).astype(out_ref.dtype)
    for swap in (qswap, nswap, kswap, vswap, fswap):
        swap.wait_send()
    for s in range(2):
        all_of(qbuf.at[s, 0 : n * n - 1], send_sem.at[outs["ag", s]])
        for g in range(GROUPS):
            all_of(obuf.at[s * GROUPS + g, 0 : n - 1], send_sem.at[outs["p3", g, s]])
        for b, (g0, g1) in enumerate(BATCHES):
            part = pl.ds(g0 * per4, (g1 - g0) * per4)
            all_of(got.at[s, 0 : n - 1, part, :], send_sem.at[outs["p4", b, s]])


def per_device(queries, cache_keys, cache_values, new_keys, new_values, valid_frames):
    ny, nx, _ = RING
    tok, heads, dim = queries.shape
    cached = cache_keys.shape[0]
    assert cached == FRAME and ny == nx == 8
    half = heads // 2
    per = half // (2 * GROUPS)
    chip_tok = 2 * tok
    total = ny * nx * chip_tok
    rows = nx * chip_tok
    ids, outs = plan()
    bf16, i16, f32 = jnp.bfloat16, jnp.int16, jnp.float32
    vmem = pltpu.VMEM
    return pl.pallas_call(
        kernel,
        name="stream_attention",
        out_shape=jax.ShapeDtypeStruct((tok, heads, dim), jnp.bfloat16),
        in_specs=[pl.BlockSpec(memory_space=pltpu.SMEM)]
        + [pl.BlockSpec(memory_space=pl.ANY)] * 5,
        out_specs=pl.BlockSpec(memory_space=pltpu.VMEM),
        scratch_shapes=[
            vmem((2, tok, heads, dim), bf16),
            vmem((2, 2, tok, heads, dim), bf16),
            vmem((cached, heads, dim), bf16),
            vmem((cached, heads, dim), bf16),
            vmem((heads, cached, dim), bf16),
            vmem((heads, cached, dim), bf16),
            vmem((half, cached, dim), bf16),
            vmem((half, cached, dim), bf16),
            vmem((2, heads, 128, dim), bf16),
            vmem((heads, chip_tok, dim), bf16),
            vmem((2, ny * nx, half // 2, chip_tok, dim), bf16),
            vmem((2, total, 2 * cached + 128), f32),
            vmem((2, total, 2 * cached + 128), bf16),
            vmem((2 * GROUPS, ny, per * rows + 8, dim), i16),
            vmem((3, 2 * GROUPS, ny, 8, 128), f32),
            vmem((2 * GROUPS, ny, 2, 8, 128), f32),
            vmem((2 * GROUPS * len(ROUTES), per * rows + 8, dim), i16),
            vmem((2, nx, GROUPS * (per * chip_tok + 8), dim), i16),
            vmem((2, nx - 1, GROUPS * (per * chip_tok + 8), dim), i16),
            vmem((half, chip_tok, dim), f32),
            vmem((2, tok, half, dim), f32),
            pltpu.SemaphoreType.DMA((len(outs),)),
            pltpu.SemaphoreType.DMA((len(ids),)),
            pltpu.SemaphoreType.DMA((5,)),
        ],
        compiler_params=pltpu.CompilerParams(
            collective_id=0, has_side_effects=True, vmem_limit_bytes=60 * 1024 * 1024
        ),
    )(valid_frames, queries, cache_keys, cache_values, new_keys, new_values)


def solution(mesh):
    torus = Mesh(mesh.devices.reshape(mesh.shape["grp"], *RING), GRP_KV)
    return jax.shard_map(
        per_device,
        mesh=torus,
        in_specs=(P(GRP_KV, None, None),) * 5 + (P("grp"),),
        out_specs=P(GRP_KV, None, None),
        check_vma=False,
    )
```
